32 devices in a mesh: gz: 2 (over x), gy: 4 (over y, core), gx: 4 (over z).
Axes of the slice: x: 2, y: 2, z: 4, core: 2. Of those that a mesh axis runs over, the one named last changes fastest.
Arguments:
- density: float32 [32, 64, 256], P('gx', 'gy', 'gz'), may hold values from 0.05 to 0.95
- spread: float32 [32, 64, 256], P('gx', 'gy', 'gz'), may hold values from 0.05 to 0.3
- sensitivities: float32 [9, 32, 64, 256], P(None, 'gx', 'gy', 'gz'), may hold values from -180 to 180, as said below
- violation: float32 [9], replicated, may hold values from -0.05 to 0.15
- multipliers_start: float32 [9], replicated, may hold values from 0.1 to 10
Outputs:
- new_density: float32 [32, 64, 256], P('gx', 'gy', 'gz')
- multipliers: float32 [9], replicated
The draws below stay inside these ranges and needn't reach their ends.
Inputs may be any that keep to these rules, and one draw needn't show every extreme that they name: `sensitivities`: Real-valued, independent from voxel to voxel.
All inputs are finite; a program needn't handle non-finite values.
Results may differ from the reference program's by a relative error of at most 0.0003.
Values sent between devices are 32-bit elements; how exact they have to be, the bound alone decides.
A program may use at most 64 MiB of HBM per device.

```python
import math
import jax
import jax.numpy as jnp
from jax import lax

FIELDS = 9
ITERS = 3
NX = 32
NY = 64
NZ = 256


def draw_sensitivities(key, part):
    key_rough = jax.random.fold_in(key, 11)
    key_scale = jax.random.fold_in(key, 12)
    ramp = 1.0 + 2.0 * jnp.arange(NX, dtype=jnp.float32) / max(NX - 1, 1)
    scales = jnp.exp(jax.random.uniform(key_scale, (FIELDS,), jnp.float32, 0.0, math.log(10.0)))
    values = jnp.clip(jax.random.normal(key_rough, (FIELDS, NX, NY, NZ), jnp.float32), -6.0, 6.0)
    return values * scales[:, None, None, None] * ramp[None, :, None, None]


def levels(rng, extent, cuts, smallest, largest):
    def one(axis_at, blocks):
        steps = jax.random.uniform(jax.random.fold_in(jax.random.fold_in(rng, 6), axis_at), (blocks,), jnp.float32, smallest / len(cuts), largest / len(cuts))
        return jnp.repeat(jnp.exp(steps), extent[axis_at] // blocks).reshape((-1,) + (1,) * (len(extent) - axis_at - 1))

    factor_of = one(*cuts[0])
    for cut in cuts[1:]:
        factor_of = factor_of * one(*cut)
    return factor_of


def setup_inputs(seed: int = 0) -> dict:
    keys = jax.random.split(jax.random.key(seed), 6)
    return {
        "density": jnp.clip(0.05 + 0.9 * jax.random.uniform(keys[0], (NX, NY, NZ), jnp.float32) ** levels(keys[0], (NX, NY, NZ), ((0, 4), (1, 4), (2, 2)), -0.2, 0.2), 0.05, 0.95),
        "spread": jnp.clip(jnp.exp(math.log(0.3) - 1.7917595 * jax.random.uniform(keys[1], (NX, NY, NZ), jnp.float32) ** levels(keys[1], (NX, NY, NZ), ((0, 4), (1, 4), (2, 2)), -0.2, 0.2)), 0.05, 0.3),
        "sensitivities": draw_sensitivities(jax.random.fold_in(keys[5], 71), 0),
        "violation": jnp.clip(jax.random.uniform(keys[3], (FIELDS,), jnp.float32, -0.05, 0.15), -0.05, 0.15),
        "multipliers_start": jnp.clip(jnp.exp(jax.random.uniform(keys[4], (FIELDS,), jnp.float32, math.log(0.1), math.log(10.0))), 0.1, 10.0),
    }


RADIUS = 3.0
RAA = 1e-05
MOVE = 0.9
REG = 0.001
FLOOR = 0.2

def smooth(padded, nx, ny, nz):
    total = None
    for a in (-1, 0, 1):
        for b in (-1, 0, 1):
            for c in (-1, 0, 1):
                weight = RADIUS - math.sqrt(a * a + b * b + c * c)
                piece = padded[..., 1 + a:1 + a + nx, 1 + b:1 + b + ny, 1 + c:1 + c + nz]
                total = weight * piece if total is None else total + weight * piece
    return total

def reference(density, spread, sensitivities, violation, multipliers_start):
    nx, ny, nz = density.shape
    denom = smooth(jnp.pad(jnp.ones_like(density), 1), nx, ny, nz)

    def one_field(field):
        return smooth(jnp.pad(field, 1), nx, ny, nz) / denom
    filtered = lax.map(one_field, sensitivities)
    cells = nx * ny * nz
    dens = density.reshape(-1)
    span = spread.reshape(-1)
    rows = jnp.concatenate([filtered.reshape(FIELDS, cells), jnp.ones((1, cells), density.dtype)], axis=0)
    grow = jnp.maximum(rows, 0.0)
    fall = jnp.maximum(-rows, 0.0)
    square = span * span
    pp = square * (1.001 * grow + 0.001 * fall + RAA)
    qq = square * (0.001 * grow + 1.001 * fall + RAA)
    lower = dens - span
    upper = dens + span
    floor_x = jnp.maximum(0.0, dens - MOVE * span)
    ceil_x = jnp.minimum(1.0, dens + MOVE * span)
    base = (pp[1:] + qq[1:]) / span
    bound = (1.0 - violation) * lax.optimization_barrier(jnp.sum(base, axis=1))

    def respond(lam):
        weights = jnp.concatenate([jnp.ones((1,), lam.dtype), lam])
        big_p = jnp.dot(weights, pp, precision=lax.Precision.HIGHEST)
        big_q = jnp.dot(weights, qq, precision=lax.Precision.HIGHEST)
        root_p = jnp.sqrt(big_p)
        root_q = jnp.sqrt(big_q)
        moved = (root_p * lower + root_q * upper) / (root_p + root_q)
        return (jnp.clip(moved, floor_x, ceil_x), big_p, big_q)
    lam = multipliers_start
    for step in range(ITERS):
        moved, big_p, big_q = respond(lam)
        above = upper - moved
        below = moved - lower
        gradient = lax.optimization_barrier(jnp.sum(pp[1:] / above + qq[1:] / below, axis=1)) - bound
        slopes = pp[1:] / (above * above) - qq[1:] / (below * below)
        curv = 2.0 * big_p / (above * above * above) + 2.0 * big_q / (below * below * below)
        schur = jnp.dot(slopes / curv, slopes.T, precision=lax.Precision.HIGHEST)
        shift = REG * jnp.trace(schur) / FIELDS
        system = schur + shift * jnp.eye(FIELDS, dtype=schur.dtype)
        factor = jnp.linalg.cholesky(system)
        delta = jax.scipy.linalg.cho_solve((factor, True), gradient)
        lam = jnp.maximum(lam + delta, FLOOR * lam)
    moved, big_p, big_q = respond(lam)
    return (moved.reshape(nx, ny, nz), lam)
```

```python
import functools
import math

import jax
import jax.numpy as jnp
from jax import lax
from jax.experimental import pallas as pl
from jax.experimental.pallas import tpu as pltpu
from jax.sharding import PartitionSpec as P

FIELDS = 9
ITERS = 3

RADIUS = 3.0
RAA = 1e-05
MOVE = 0.9
REG = 0.001
FLOOR = 0.2

W0 = RADIUS
W1 = RADIUS - 1.0
W2 = RADIUS - math.sqrt(2.0)
W3 = RADIUS - math.sqrt(3.0)

SUB, LANE = 8, 128
AXES = ("gz", "gy", "gx")
SUMS = FIELDS + FIELDS * (FIELDS + 1) // 2
ROWS = SUMS + FIELDS
MESH = pl.DeviceIdType.MESH


def plan(shape):
    total = math.prod(shape[a] for a in AXES)
    if total <= 32:
        return (AXES,)
    return tuple((a,) for a in AXES)


def offsets(axes, shape):
    out = [()]
    for a in axes:
        out = [o + (d,) for o in out for d in range(shape[a])]
    return [o for o in out if any(o)]


def body(shape, dims, dens_ref, span_ref, sens_ref, viol_ref, lam0_ref, out_ref, lam_out,
         pad, ypack, yrecv, cpack, crecv, zsum, zpack, zrecv, mid, invden, pp, qq, slope, scaled,
         acc, wide, lam, part, *rest):
    stages = plan(shape)
    recvs = rest[: len(stages)]
    load_sem, send_sem, recv_sem, sum_send, sum_recv = rest[len(stages):]
    nx, ny, nz = dims
    tiles = ny // SUB
    chunks = nx * tiles
    me = {a: lax.axis_index(a) for a in AXES}

    load = pltpu.make_async_copy(
        sens_ref, pad.at[:, 1 : nx + 1, SUB : SUB + ny, :], load_sem
    )
    load.start()

    partners = set()
    for axes in stages:
        for o in offsets(axes, shape):
            partners.add(tuple(dict(zip(axes, o)).get(a, 0) for a in AXES))
    for dz, dy, dx in [(dz, 0, 0) for dz in (-1, 1)] + [
        (0, dy, dx) for dy in (-1, 0, 1) for dx in (-1, 0, 1)
    ]:
        o = tuple(d % shape[a] for a, d in zip(AXES, (dz, dy, dx)))
        if any(o):
            partners.add(o)
    partners = sorted(partners)
    barrier = pltpu.get_barrier_semaphore()
    for o in partners:
        target = {a: lax.rem(me[a] + d, shape[a]) for a, d in zip(AXES, o)}
        pl.semaphore_signal(barrier, inc=1, device_id=target, device_id_type=MESH)

    has = {}
    for a in AXES:
        has[a, -1] = me[a] > 0
        has[a, 1] = me[a] < shape[a] - 1

    lane = lax.broadcasted_iota(jnp.int32, (SUB, LANE), 1)
    row = lax.broadcasted_iota(jnp.int32, (SUB, LANE), 0)
    zero = jnp.zeros((SUB, LANE), jnp.float32)

    for i, sx in enumerate((1, -1)):
        @pl.when(jnp.logical_not(has["gx", -sx]))
        def _(i=i):
            pad[:, i * (nx + 1), SUB : SUB + ny, :] = jnp.zeros((FIELDS, ny, LANE), jnp.float32)
    for i, sy in enumerate((1, -1)):
        @pl.when(jnp.logical_not(has["gy", -sy]))
        def _(i=i):
            yrecv[i] = jnp.zeros((FIELDS, nx, LANE), jnp.float32)
    for i, sz in enumerate((1, -1)):
        @pl.when(jnp.logical_not(has["gz", -sz]))
        def _(i=i):
            zrecv[i] = jnp.zeros(zrecv.shape[1:], jnp.float32)
    corners = [(sx, sy) for sx in (1, -1) for sy in (1, -1)]
    for i, (sx, sy) in enumerate(corners):
        @pl.when(jnp.logical_not(jnp.logical_and(has["gx", -sx], has["gy", -sy])))
        def _(i=i):
            crecv[i] = jnp.zeros((FIELDS, 1, LANE), jnp.float32)
    zsum[...] = jnp.zeros(zsum.shape, jnp.float32)

    def count(a, index, extent):
        low = jnp.where(jnp.logical_and(me[a] == 0, index == 0), 0.0, 1.0)
        high = jnp.where(jnp.logical_and(me[a] == shape[a] - 1, index == extent - 1), 0.0, 1.0)
        return low + high
    cz = count("gz", lane, nz)
    for x in range(nx):
        cx = count("gx", jnp.full((SUB, LANE), x, jnp.int32), nx)
        for t in range(tiles):
            cy = count("gy", row + t * SUB, ny)
            den = W0 + W1 * (cx + cy + cz) + W2 * (cx * cy + cy * cz + cx * cz) + W3 * (cx * cy * cz)
            k = x * tiles + t
            invden[k] = 1.0 / den

    load.wait()

    def gather(f, carry):
        for i, y in enumerate((SUB + ny - 1, SUB)):
            for x in range(nx):
                ypack[i, f, x : x + 1, :] = pad[f, x + 1, y : y + 1, :]
        for i, (sx, sy) in enumerate(corners):
            x = nx if sx > 0 else 1
            y = SUB + ny - 1 if sy > 0 else SUB
            cpack[i, f] = pad[f, x, y : y + 1, :]
        return carry
    lax.fori_loop(0, FIELDS, gather, 0)

    pl.semaphore_wait(barrier, len(partners))

    def at(**moves):
        return {a: me[a] + d for a, d in moves.items()}

    moves = []
    for i, sx in enumerate((1, -1)):
        copy = pltpu.make_async_remote_copy(
            src_ref=pad.at[:, nx if sx > 0 else 1, SUB : SUB + ny, :],
            dst_ref=pad.at[:, 0 if sx > 0 else nx + 1, SUB : SUB + ny, :],
            send_sem=send_sem.at[i], recv_sem=recv_sem.at[i],
            device_id=at(gx=sx), device_id_type=MESH)
        moves.append((has["gx", sx], has["gx", -sx], copy))
    for i, (sx, sy) in enumerate(corners):
        copy = pltpu.make_async_remote_copy(
            src_ref=cpack.at[i], dst_ref=crecv.at[i],
            send_sem=send_sem.at[4 + i], recv_sem=recv_sem.at[4 + i],
            device_id=at(gx=sx, gy=sy), device_id_type=MESH)
        moves.append((jnp.logical_and(has["gx", sx], has["gy", sy]),
                      jnp.logical_and(has["gx", -sx], has["gy", -sy]), copy))
    for i, sy in enumerate((1, -1)):
        copy = pltpu.make_async_remote_copy(
            src_ref=ypack.at[i], dst_ref=yrecv.at[i],
            send_sem=send_sem.at[2 + i], recv_sem=recv_sem.at[2 + i],
            device_id=at(gy=sy), device_id_type=MESH)
        moves.append((has["gy", sy], has["gy", -sy], copy))
    for send, _, copy in moves:
        pl.when(send)(copy.start)
    for _, receive, copy in moves:
        pl.when(receive)(copy.wait_recv)

    ends = jnp.logical_or(lane == 0, lane == LANE - 1)

    def smooth(f, carry):
        for i, y in enumerate((SUB - 1, SUB + ny)):
            for x in range(nx):
                pad[f, x + 1, y : y + 1, :] = yrecv[i, f, x : x + 1, :]
        for i, (sx, sy) in enumerate(corners):
            pad[f, 0 if sx > 0 else nx + 1, (SUB - 1 if sy > 0 else SUB + ny) : (SUB if sy > 0 else SUB + ny + 1), :] = crecv[i, f]
        packed = zero
        for t in range(tiles):
            y = SUB + t * SUB
            mids, sides = [], []
            for p in range(nx + 2):
                mids.append(pad[f, p, y : y + SUB, :])
                sides.append(pad[f, p, y - 1 : y - 1 + SUB, :] + pad[f, p, y + 1 : y + 1 + SUB, :])
            for x in range(nx):
                k = x * tiles + t
                near = sides[x + 1] + (mids[x] + mids[x + 2])
                far = sides[x] + sides[x + 2]
                s0 = W0 * mids[x + 1] + W1 * near + W2 * far
                s1 = W1 * mids[x + 1] + W2 * near + W3 * far
                up = pltpu.roll(s1, 1, 1)
                down = pltpu.roll(s1, LANE - 1, 1)
                mid[f, k] = s0 + jnp.where(lane == 0, 0.0, up) + jnp.where(lane == LANE - 1, 0.0, down)
                edge = jnp.where(lane == 0, up, down)
                if k:
                    edge = pltpu.roll(edge, 2 * k, 1)
                here = jnp.logical_or(lane == 2 * k, lane == (2 * k - 1) % LANE)
                packed = jnp.where(here, edge, packed)
        zsum[f // per] += pltpu.roll(packed, (f % per) * (2 * chunks), 1)
        return carry
    per = LANE // (2 * chunks)
    lax.fori_loop(0, FIELDS, smooth, 0)

    even = (lane % 2) == 0
    for g in range(zsum.shape[0]):
        v = zsum[g]
        zpack[0, g] = jnp.where(even, v, 0.0)
        zpack[1, g] = jnp.where(even, 0.0, v)
    zmoves = []
    for i, sz in enumerate((1, -1)):
        copy = pltpu.make_async_remote_copy(
            src_ref=zpack.at[i], dst_ref=zrecv.at[i],
            send_sem=send_sem.at[8 + i], recv_sem=recv_sem.at[8 + i],
            device_id=at(gz=sz), device_id_type=MESH)
        zmoves.append((has["gz", sz], has["gz", -sz], copy))
    for send, _, copy in zmoves:
        pl.when(send)(copy.start)
    for _, receive, copy in zmoves:
        pl.when(receive)(copy.wait_recv)

    def piece(ref, k):
        x, t = divmod(k, tiles)
        return ref[x, t * SUB : (t + 1) * SUB, :]

    def rows(f, carry):
        outer = zrecv[0, f // per] + zrecv[1, f // per]
        outer = pltpu.roll(outer, lax.rem(LANE - (f % per) * (2 * chunks), LANE), 1)
        total = zero
        for k in range(chunks):
            edge = pltpu.roll(outer, LANE - 2 * k, 1) if k else outer
            r = (mid[f, k] + jnp.where(ends, edge, 0.0)) * invden[k]
            s = piece(span_ref, k)
            square = s * s
            gp = jnp.maximum(r, 0.0)
            gm = jnp.maximum(-r, 0.0)
            pp[f, k] = square * (1.001 * gp + 0.001 * gm + RAA)
            qq[f, k] = square * (0.001 * gp + 1.001 * gm + RAA)
            total += s * (1.002 * (gp + gm) + 2 * RAA)
        acc[SUMS - 1 + f] = jnp.where(f > 0, total, zero)
        return carry
    lax.fori_loop(0, FIELDS, rows, 0)
    total = zero
    for k in range(chunks):
        s = piece(span_ref, k)
        square = s * s
        pp[FIELDS, k] = square * (1.001 + RAA)
        qq[FIELDS, k] = square * (0.001 + RAA)
        total += s * (1.002 + 2 * RAA)
    acc[ROWS - 1] = total
    for k in range(FIELDS):
        lam[k] = jnp.full((SUB, LANE), lam0_ref[k], jnp.float32)

    def respond(k, weights):
        big_p, big_q = pp[0, k], qq[0, k]
        for j in range(FIELDS):
            big_p += weights[j] * pp[j + 1, k]
            big_q += weights[j] * qq[j + 1, k]
        s = piece(span_ref, k)
        d = piece(dens_ref, k)
        root_p = jnp.sqrt(big_p)
        root_q = jnp.sqrt(big_q)
        lower, upper = d - s, d + s
        moved = (root_p * lower + root_q * upper) / (root_p + root_q)
        low = jnp.maximum(0.0, d - MOVE * s)
        high = jnp.minimum(1.0, d + MOVE * s)
        return jnp.minimum(jnp.maximum(moved, low), high), big_p, big_q, lower, upper

    def flat(axes):
        index = 0
        for a in axes:
            index = index * shape[a] + me[a]
        return index

    def newton(it, carry):
        weights = [lam[j] for j in range(FIELDS)]
        grads = [zero] * FIELDS
        for k in range(chunks):
            moved, big_p, big_q, lower, upper = respond(k, weights)
            ia = 1.0 / (upper - moved)
            ib = 1.0 / (moved - lower)
            ia2, ib2 = ia * ia, ib * ib
            inv = 1.0 / (2.0 * big_p * (ia2 * ia) + 2.0 * big_q * (ib2 * ib))
            for j in range(FIELDS):
                p, q = pp[j + 1, k], qq[j + 1, k]
                grads[j] += p * ia + q * ib
                a = p * ia2 - q * ib2
                slope[j, k] = a
                scaled[j, k] = a * inv
        for j in range(FIELDS):
            acc[j] = grads[j]
        at_row = FIELDS
        for group in ((0, 1), (2, 3), (4, 5, 6, 7, 8)):
            sums = {(i, j): zero for i in group for j in range(i, FIELDS)}
            for k in range(chunks):
                right = {j: slope[j, k] for j in range(group[0], FIELDS)}
                for i in group:
                    left = scaled[i, k]
                    for j in range(i, FIELDS):
                        sums[i, j] += left * right[j]
            for key in sums:
                acc[at_row] = sums[key]
                at_row += 1

        packed = zero
        for r in range(ROWS):
            packed = jnp.where(lane == r, jnp.sum(acc[r], axis=1, keepdims=True), packed)
        value = jnp.sum(packed, axis=0, keepdims=True)
        for n, axes in enumerate(stages):
            size = math.prod(shape[a] for a in axes)
            part[it, n] = value
            recvs[n][it, flat(axes)] = value
            for o in offsets(axes, shape):
                target = {a: lax.rem(me[a] + d, shape[a]) for a, d in zip(axes, o)}
                pltpu.make_async_remote_copy(
                    src_ref=part.at[it, n], dst_ref=recvs[n].at[it, flat(axes)],
                    send_sem=sum_send.at[it, n], recv_sem=sum_recv.at[it, n],
                    device_id=target, device_id_type=MESH).start()
            whole = recvs[n].at[it, pl.ds(0, size - 1)]
            pltpu.make_async_copy(whole, whole, sum_recv.at[it, n]).wait()
            values = [recvs[n][it, i] for i in range(size)]
            while len(values) > 1:
                values = [sum(values[i + 1 : i + 2], values[i]) for i in range(0, len(values), 2)]
            value = values[0]
        every = jnp.broadcast_to(value, (SUB, LANE))
        for g in range(wide.shape[0]):
            one = jnp.sum(jnp.where(lane == g * SUB + row, every, 0.0), axis=1, keepdims=True)
            wide[g] = jnp.broadcast_to(one, (SUB, LANE))

        def read(r):
            return jnp.broadcast_to(wide[r // SUB, r % SUB : r % SUB + 1, :], (SUB, LANE))
        b = [read(j) - (1.0 - viol_ref[j]) * read(SUMS + j) for j in range(FIELDS)]
        m = {}
        at_row = FIELDS
        for i in range(FIELDS):
            for j in range(i, FIELDS):
                m[i, j] = read(at_row)
                at_row += 1
        trace = m[0, 0]
        for i in range(1, FIELDS):
            trace += m[i, i]
        shift = REG * trace / FIELDS
        for i in range(FIELDS):
            m[i, i] += shift
        inverse = []
        for k in range(FIELDS):
            inverse.append(1.0 / m[k, k])
            for i in range(k + 1, FIELDS):
                factor = m[k, i] * inverse[k]
                for j in range(i, FIELDS):
                    m[i, j] -= factor * m[k, j]
                b[i] -= factor * b[k]
        delta = [None] * FIELDS
        for k in reversed(range(FIELDS)):
            v = b[k]
            for j in range(k + 1, FIELDS):
                v -= m[k, j] * delta[j]
            delta[k] = v * inverse[k]
        for k in range(FIELDS):
            lam[k] = jnp.maximum(weights[k] + delta[k], FLOOR * weights[k])
        return carry
    lax.fori_loop(0, ITERS, newton, 0)

    weights = [lam[j] for j in range(FIELDS)]
    for k in range(chunks):
        x, t = divmod(k, tiles)
        out_ref[x, t * SUB : (t + 1) * SUB, :] = respond(k, weights)[0]
    for j in range(FIELDS):
        lam_out[j] = jnp.max(weights[j])

    for send, _, copy in moves + zmoves:
        pl.when(send)(copy.wait_send)
    for it in range(ITERS):
        for n, axes in enumerate(stages):
            size = math.prod(shape[a] for a in axes)
            whole = recvs[n].at[it, pl.ds(0, size - 1)]
            pltpu.make_async_copy(whole, whole, sum_send.at[it, n]).wait()


def shards(shape, density, spread, sensitivities, violation, multipliers_start):
    nx, ny, nz = density.shape
    chunks = nx * ny // SUB
    per = LANE // (2 * chunks)
    groups = -(-FIELDS // per)
    stages = plan(shape)
    f32 = jnp.float32
    vmem = pl.BlockSpec(memory_space=pltpu.VMEM)
    smem = pl.BlockSpec(memory_space=pltpu.SMEM)
    dma = pltpu.SemaphoreType.DMA
    return pl.pallas_call(
        functools.partial(body, shape, (nx, ny, nz)),
        out_shape=(
            jax.ShapeDtypeStruct((nx, ny, nz), f32),
            jax.ShapeDtypeStruct((FIELDS,), f32),
        ),
        in_specs=[vmem, vmem, pl.BlockSpec(memory_space=pl.ANY), smem, smem],
        out_specs=(vmem, smem),
        scratch_shapes=[
            pltpu.VMEM((FIELDS, nx + 2, ny + 2 * SUB, nz), f32),
            pltpu.VMEM((2, FIELDS, nx, nz), f32),
            pltpu.VMEM((2, FIELDS, nx, nz), f32),
            pltpu.VMEM((4, FIELDS, 1, nz), f32),
            pltpu.VMEM((4, FIELDS, 1, nz), f32),
            pltpu.VMEM((groups, SUB, LANE), f32),
            pltpu.VMEM((2, groups, SUB, LANE), f32),
            pltpu.VMEM((2, groups, SUB, LANE), f32),
            pltpu.VMEM((FIELDS, chunks, SUB, LANE), f32),
            pltpu.VMEM((chunks, SUB, LANE), f32),
            pltpu.VMEM((FIELDS + 1, chunks, SUB, LANE), f32),
            pltpu.VMEM((FIELDS + 1, chunks, SUB, LANE), f32),
            pltpu.VMEM((FIELDS, chunks, SUB, LANE), f32),
            pltpu.VMEM((FIELDS, chunks, SUB, LANE), f32),
            pltpu.VMEM((ROWS, SUB, LANE), f32),
            pltpu.VMEM((-(-ROWS // SUB), SUB, LANE), f32),
            pltpu.VMEM((FIELDS, SUB, LANE), f32),
            pltpu.VMEM((ITERS, len(stages), 1, LANE), f32),
        ] + [
            pltpu.VMEM((ITERS, math.prod(shape[a] for a in axes), 1, LANE), f32) for axes in stages
        ] + [
            dma, dma((10,)), dma((10,)), dma((ITERS, len(stages))), dma((ITERS, len(stages))),
        ],
        compiler_params=pltpu.CompilerParams(collective_id=0, has_side_effects=True),
        name="design_step",
    )(density, spread, sensitivities, violation, multipliers_start)


def solution(mesh):
    shape = {a: int(mesh.shape[a]) for a in AXES}
    return jax.shard_map(
        functools.partial(shards, shape),
        mesh=mesh,
        in_specs=(P("gx", "gy", "gz"), P("gx", "gy", "gz"), P(None, "gx", "gy", "gz"), P(), P()),
        out_specs=(P("gx", "gy", "gz"), P()),
        check_vma=False,
    )
```

```python
import functools
import math

import jax
import jax.numpy as jnp
from jax import lax
from jax.experimental import pallas as pl
from jax.experimental.pallas import tpu as pltpu
from jax.sharding import PartitionSpec as P

FIELDS = 9
ITERS = 3

RADIUS = 3.0
RAA = 1e-05
MOVE = 0.9
REG = 0.001
FLOOR = 0.2

W0 = RADIUS
W1 = RADIUS - 1.0
W2 = RADIUS - math.sqrt(2.0)
W3 = RADIUS - math.sqrt(3.0)

SUB, LANE = 8, 128
AXES = ("gz", "gy", "gx")
SUMS = FIELDS + FIELDS * (FIELDS + 1) // 2
ROWS = SUMS + FIELDS
MESH = pl.DeviceIdType.MESH
GROUP = 3


def plan(shape):
    total = math.prod(shape[a] for a in AXES)
    if total <= 32:
        return (AXES,)
    return tuple((a,) for a in AXES)


def offsets(axes, shape):
    out = [()]
    for a in axes:
        out = [o + (d,) for o in out for d in range(shape[a])]
    return [o for o in out if any(o)]


def steps():
    return [range(f, min(f + GROUP, FIELDS)) for f in range(0, FIELDS, GROUP)]


def body(shape, dims, dens_hbm, span_hbm, sens_ref, viol_hbm, lam0_hbm, out_hbm, lam_out,
         dens_ref, span_ref, out_ref, viol_ref, lam0_ref, pad, ypack, yrecv, cpack, crecv, zpack, zrecv, mid, invden, pp, qq, slope, scaled,
         acc, wide, lam, part, *rest):
    stages = plan(shape)
    recvs = rest[: len(stages)]
    load_sem, send_sem, recv_sem, sum_send, sum_recv, known = rest[len(stages):]
    nx, ny, nz = dims
    tiles = ny // SUB
    chunks = nx * tiles
    me = {a: lax.axis_index(a) for a in AXES}

    has = {}
    for a in AXES:
        has[a, -1] = me[a] > 0
        has[a, 0] = jnp.bool_(True)
        has[a, 1] = me[a] < shape[a] - 1

    def both(o):
        moved = [has[a, d] for a, d in zip(AXES, o) if d]
        return functools.reduce(jnp.logical_and, moved)

    def at(**moves):
        return {a: me[a] + d for a, d in moves.items()}

    plane = [(0, dy, dx) for dy in (-1, 0, 1) for dx in (-1, 0, 1) if dy or dx]
    barrier = pltpu.get_barrier_semaphore()
    near = shape["gz"] == 2 and shape["gy"] <= 4 and shape["gx"] <= 4
    if near:
        greeted = [(-1, 0, 0), (1, 0, 0)] + plane
        for o in greeted:
            @pl.when(both(o))
            def _(o=o):
                pl.semaphore_signal(barrier, inc=1, device_id=at(gz=o[0], gy=o[1], gx=o[2]),
                                    device_id_type=MESH)
        arrivals = sum(both(o).astype(jnp.int32) for o in greeted)
    else:
        partners = set()
        for axes in stages:
            for o in offsets(axes, shape):
                partners.add(tuple(dict(zip(axes, o)).get(a, 0) for a in AXES))
        for d in [(-1, 0, 0), (1, 0, 0)] + plane:
            o = tuple(d % shape[a] for a, d in zip(AXES, d))
            if any(o):
                partners.add(o)
        partners = sorted(partners)
        for o in partners:
            target = {a: lax.rem(me[a] + d, shape[a]) for a, d in zip(AXES, o)}
            pl.semaphore_signal(barrier, inc=1, device_id=target, device_id_type=MESH)
        arrivals = len(partners)

    load = pltpu.make_async_copy(
        sens_ref, pad.at[:, 1 : nx + 1, SUB : SUB + ny, :], load_sem.at[0]
    )
    load.start()
    small = [
        pltpu.make_async_copy(src, dst, load_sem.at[1 + i])
        for i, (src, dst) in enumerate([
            (span_hbm, span_ref), (dens_hbm, dens_ref), (viol_hbm, viol_ref), (lam0_hbm, lam0_ref)])
    ]
    for copy in small:
        copy.start()

    lane = lax.broadcasted_iota(jnp.int32, (SUB, LANE), 1)
    row = lax.broadcasted_iota(jnp.int32, (SUB, LANE), 0)
    zero = jnp.zeros((SUB, LANE), jnp.float32)

    for i, sx in enumerate((1, -1)):
        @pl.when(jnp.logical_not(has["gx", -sx]))
        def _(i=i):
            pad[:, i * (nx + 1), SUB : SUB + ny, :] = jnp.zeros((FIELDS, ny, LANE), jnp.float32)
    for i, sy in enumerate((1, -1)):
        @pl.when(jnp.logical_not(has["gy", -sy]))
        def _(i=i):
            yrecv[i] = jnp.zeros((FIELDS, nx, LANE), jnp.float32)
    for i, sz in enumerate((1, -1)):
        @pl.when(jnp.logical_not(has["gz", -sz]))
        def _(i=i):
            zrecv[i] = jnp.zeros(zrecv.shape[1:], jnp.float32)
    corners = [(sx, sy) for sx in (1, -1) for sy in (1, -1)]
    for i, (sx, sy) in enumerate(corners):
        @pl.when(jnp.logical_not(jnp.logical_and(has["gx", -sx], has["gy", -sy])))
        def _(i=i):
            crecv[i] = jnp.zeros((FIELDS, 1, LANE), jnp.float32)

    def count(a, index, extent):
        low = jnp.where(jnp.logical_and(me[a] == 0, index == 0), 0.0, 1.0)
        high = jnp.where(jnp.logical_and(me[a] == shape[a] - 1, index == extent - 1), 0.0, 1.0)
        return low + high
    cz = count("gz", lane, nz)
    for x in range(nx):
        cx = count("gx", jnp.full((SUB, LANE), x, jnp.int32), nx)
        for t in range(tiles):
            cy = count("gy", row + t * SUB, ny)
            den = W0 + W1 * (cx + cy + cz) + W2 * (cx * cy + cy * cz + cx * cz) + W3 * (cx * cy * cz)
            k = x * tiles + t
            invden[k] = 1.0 / den

    load.wait()

    for f in range(FIELDS):
        for i, y in enumerate((SUB + ny - 1, SUB)):
            for x in range(nx):
                ypack[i, f, x : x + 1, :] = pad[f, x + 1, y : y + 1, :]
        for i, (sx, sy) in enumerate(corners):
            x = nx if sx > 0 else 1
            y = SUB + ny - 1 if sy > 0 else SUB
            cpack[i, f] = pad[f, x, y : y + 1, :]

    pl.semaphore_wait(barrier, arrivals)

    groups = steps()
    count_of = len(groups)

    def moves_x(g):
        fields = pl.ds(groups[g][0], len(groups[g]))
        out = []
        for i, sx in enumerate((1, -1)):
            copy = pltpu.make_async_remote_copy(
                src_ref=pad.at[fields, nx if sx > 0 else 1, SUB : SUB + ny, :],
                dst_ref=pad.at[fields, 0 if sx > 0 else nx + 1, SUB : SUB + ny, :],
                send_sem=send_sem.at[6 + 4 * g + i], recv_sem=recv_sem.at[6 + 4 * g + i],
                device_id=at(gx=sx), device_id_type=MESH)
            out.append((has["gx", sx], has["gx", -sx], copy))
        return out

    moves_c, moves_y, moves_z = [], [], []
    for i, (sx, sy) in enumerate(corners):
        copy = pltpu.make_async_remote_copy(
            src_ref=cpack.at[i], dst_ref=crecv.at[i],
            send_sem=send_sem.at[2 + i], recv_sem=recv_sem.at[2 + i],
            device_id=at(gx=sx, gy=sy), device_id_type=MESH)
        moves_c.append((jnp.logical_and(has["gx", sx], has["gy", sy]),
                        jnp.logical_and(has["gx", -sx], has["gy", -sy]), copy))
    for i, sy in enumerate((1, -1)):
        copy = pltpu.make_async_remote_copy(
            src_ref=ypack.at[i], dst_ref=yrecv.at[i],
            send_sem=send_sem.at[i], recv_sem=recv_sem.at[i],
            device_id=at(gy=sy), device_id_type=MESH)
        moves_y.append((has["gy", sy], has["gy", -sy], copy))

    def start(moves):
        for send, _, copy in moves:
            pl.when(send)(copy.start)

    def receive(moves):
        for _, expected, copy in moves:
            pl.when(expected)(copy.wait_recv)

    xs = [moves_x(g) for g in range(count_of)]
    start(moves_c)
    start(xs[0])
    start(moves_y)
    for g in range(1, count_of):
        start(xs[g])
    receive(moves_c)
    receive(moves_y)

    ends = jnp.logical_or(lane == 0, lane == LANE - 1)

    def smooth(f, g):
        for i, y in enumerate((SUB - 1, SUB + ny)):
            for x in range(nx):
                pad[f, x + 1, y : y + 1, :] = yrecv[i, f, x : x + 1, :]
        for i, (sx, sy) in enumerate(corners):
            pad[f, 0 if sx > 0 else nx + 1, (SUB - 1 if sy > 0 else SUB + ny) : (SUB if sy > 0 else SUB + ny + 1), :] = crecv[i, f]
        packed = zero
        for t in range(tiles):
            y = SUB + t * SUB
            mids, sides = [], []
            for p in range(nx + 2):
                mids.append(pad[f, p, y : y + SUB, :])
                sides.append(pad[f, p, y - 1 : y - 1 + SUB, :] + pad[f, p, y + 1 : y + 1 + SUB, :])
            for x in range(nx):
                k = x * tiles + t
                near = sides[x + 1] + (mids[x] + mids[x + 2])
                far = sides[x] + sides[x + 2]
                s0 = W0 * mids[x + 1] + W1 * near + W2 * far
                s1 = W1 * mids[x + 1] + W2 * near + W3 * far
                up = pltpu.roll(s1, 1, 1)
                down = pltpu.roll(s1, LANE - 1, 1)
                mid[f, k] = s0 + jnp.where(lane == 0, 0.0, up) + jnp.where(lane == LANE - 1, 0.0, down)
                edge = jnp.where(lane == 0, up, down)
                if k:
                    edge = pltpu.roll(edge, 2 * k, 1)
                here = jnp.logical_or(lane == 2 * k, lane == (2 * k - 1) % LANE)
                packed = jnp.where(here, edge, packed)
        shift = (f - groups[g][0]) * (2 * chunks)
        return pltpu.roll(packed, shift, 1) if shift else packed

    even = (lane % 2) == 0
    for g in range(count_of):
        receive(xs[g])
        v = zero
        for f in groups[g]:
            v += smooth(f, g)
        zpack[0, g] = jnp.where(even, v, 0.0)
        zpack[1, g] = jnp.where(even, 0.0, v)
        zs = []
        for i, sz in enumerate((1, -1)):
            copy = pltpu.make_async_remote_copy(
                src_ref=zpack.at[i, g], dst_ref=zrecv.at[i, g],
                send_sem=send_sem.at[8 + 4 * g + i], recv_sem=recv_sem.at[8 + 4 * g + i],
                device_id=at(gz=sz), device_id_type=MESH)
            zs.append((has["gz", sz], has["gz", -sz], copy))
        start(zs)
        moves_z.append(zs)

    def piece(ref, k):
        x, t = divmod(k, tiles)
        return ref[x, t * SUB : (t + 1) * SUB, :]

    def rows(f, g):
        outer = zrecv[0, g] + zrecv[1, g]
        shift = (f - groups[g][0]) * (2 * chunks)
        total = zero
        for k in range(chunks):
            turn = (LANE - shift - 2 * k) % LANE
            edge = pltpu.roll(outer, turn, 1) if turn else outer
            r = (mid[f, k] + jnp.where(ends, edge, 0.0)) * invden[k]
            s = piece(span_ref, k)
            square = s * s
            gp = jnp.maximum(r, 0.0)
            gm = jnp.maximum(-r, 0.0)
            pp[f, k] = square * (1.001 * gp + 0.001 * gm + RAA)
            qq[f, k] = square * (0.001 * gp + 1.001 * gm + RAA)
            total += s * (1.002 * (gp + gm) + 2 * RAA)
        if f:
            acc[SUMS - 1 + f] = total

    for copy in small:
        copy.wait()
    for g in range(count_of):
        receive(moves_z[g])
        if near and g == 0:
            for o in plane:
                @pl.when(both(o))
                def _(o=o):
                    pl.semaphore_signal(known, inc=1, device_id=at(gy=o[1], gx=o[2]),
                                        device_id_type=MESH)
        for f in groups[g]:
            rows(f, g)
    total = zero
    for k in range(chunks):
        s = piece(span_ref, k)
        square = s * s
        pp[FIELDS, k] = square * (1.001 + RAA)
        qq[FIELDS, k] = square * (0.001 + RAA)
        total += s * (1.002 + 2 * RAA)
    acc[ROWS - 1] = total
    for k in range(FIELDS):
        lam[k] = jnp.full((SUB, LANE), lam0_ref[k], jnp.float32)

    def respond(k, weights):
        big_p, big_q = pp[0, k], qq[0, k]
        for j in range(FIELDS):
            big_p += weights[j] * pp[j + 1, k]
            big_q += weights[j] * qq[j + 1, k]
        s = piece(span_ref, k)
        d = piece(dens_ref, k)
        root_p = jnp.sqrt(big_p)
        root_q = jnp.sqrt(big_q)
        lower, upper = d - s, d + s
        moved = (root_p * lower + root_q * upper) / (root_p + root_q)
        low = jnp.maximum(0.0, d - MOVE * s)
        high = jnp.minimum(1.0, d + MOVE * s)
        return jnp.minimum(jnp.maximum(moved, low), high), big_p, big_q, lower, upper

    def flat(axes):
        index = 0
        for a in axes:
            index = index * shape[a] + me[a]
        return index

    def newton(it, carry):
        weights = [lam[j] for j in range(FIELDS)]
        grads = [zero] * FIELDS
        for k in range(chunks):
            moved, big_p, big_q, lower, upper = respond(k, weights)
            ia = 1.0 / (upper - moved)
            ib = 1.0 / (moved - lower)
            ia2, ib2 = ia * ia, ib * ib
            inv = 1.0 / (2.0 * big_p * (ia2 * ia) + 2.0 * big_q * (ib2 * ib))
            for j in range(FIELDS):
                p, q = pp[j + 1, k], qq[j + 1, k]
                grads[j] += p * ia + q * ib
                a = p * ia2 - q * ib2
                slope[j, k] = a
                scaled[j, k] = a * inv
        for j in range(FIELDS):
            acc[j] = grads[j]
        at_row = FIELDS
        for group in ((0, 1), (2, 3), (4, 5, 6, 7, 8)):
            sums = {(i, j): zero for i in group for j in range(i, FIELDS)}
            for k in range(chunks):
                right = {j: slope[j, k] for j in range(group[0], FIELDS)}
                for i in group:
                    left = scaled[i, k]
                    for j in range(i, FIELDS):
                        sums[i, j] += left * right[j]
            for key in sums:
                acc[at_row] = sums[key]
                at_row += 1

        packed = zero
        for r in range(ROWS):
            packed = jnp.where(lane == r, jnp.sum(acc[r], axis=1, keepdims=True), packed)
        value = jnp.sum(packed, axis=0, keepdims=True)
        for n, axes in enumerate(stages):
            size = math.prod(shape[a] for a in axes)
            part[it, n] = value
            recvs[n][it, flat(axes)] = value
            for o in offsets(axes, shape):
                target = {a: lax.rem(me[a] + d, shape[a]) for a, d in zip(axes, o)}
                pltpu.make_async_remote_copy(
                    src_ref=part.at[it, n], dst_ref=recvs[n].at[it, flat(axes)],
                    send_sem=sum_send.at[it, n], recv_sem=sum_recv.at[it, n],
                    device_id=target, device_id_type=MESH).start()
            whole = recvs[n].at[it, pl.ds(0, size - 1)]
            pltpu.make_async_copy(whole, whole, sum_recv.at[it, n]).wait()
            values = [recvs[n][it, i] for i in range(size)]
            while len(values) > 1:
                values = [sum(values[i + 1 : i + 2], values[i]) for i in range(0, len(values), 2)]
            value = values[0]
        every = jnp.broadcast_to(value, (SUB, LANE))
        for g in range(wide.shape[0]):
            one = jnp.sum(jnp.where(lane == g * SUB + row, every, 0.0), axis=1, keepdims=True)
            wide[g] = jnp.broadcast_to(one, (SUB, LANE))

        def read(r):
            return jnp.broadcast_to(wide[r // SUB, r % SUB : r % SUB + 1, :], (SUB, LANE))
        b = [read(j) - (1.0 - viol_ref[j]) * read(SUMS + j) for j in range(FIELDS)]
        m = {}
        at_row = FIELDS
        for i in range(FIELDS):
            for j in range(i, FIELDS):
                m[i, j] = read(at_row)
                at_row += 1
        trace = m[0, 0]
        for i in range(1, FIELDS):
            trace += m[i, i]
        shift = REG * trace / FIELDS
        for i in range(FIELDS):
            m[i, i] += shift
        inverse = []
        for k in range(FIELDS):
            inverse.append(1.0 / m[k, k])
            for i in range(k + 1, FIELDS):
                factor = m[k, i] * inverse[k]
                for j in range(i, FIELDS):
                    m[i, j] -= factor * m[k, j]
                b[i] -= factor * b[k]
        delta = [None] * FIELDS
        for k in reversed(range(FIELDS)):
            v = b[k]
            for j in range(k + 1, FIELDS):
                v -= m[k, j] * delta[j]
            delta[k] = v * inverse[k]
        for k in range(FIELDS):
            lam[k] = jnp.maximum(weights[k] + delta[k], FLOOR * weights[k])
        return carry
    if near:
        pl.semaphore_wait(known, sum(both(o).astype(jnp.int32) for o in plane))
    lax.fori_loop(0, ITERS, newton, 0)

    weights = [lam[j] for j in range(FIELDS)]
    for k in range(chunks):
        x, t = divmod(k, tiles)
        out_ref[x, t * SUB : (t + 1) * SUB, :] = respond(k, weights)[0]
    result = pltpu.make_async_copy(out_ref, out_hbm, load_sem.at[0])
    result.start()
    for j in range(FIELDS):
        lam_out[j] = jnp.max(weights[j])

    for moves in [moves_c, moves_y] + xs + moves_z:
        for send, _, copy in moves:
            pl.when(send)(copy.wait_send)
    for it in range(ITERS):
        for n, axes in enumerate(stages):
            size = math.prod(shape[a] for a in axes)
            whole = recvs[n].at[it, pl.ds(0, size - 1)]
            pltpu.make_async_copy(whole, whole, sum_send.at[it, n]).wait()
    result.wait()


def finish(field_ref, lam_ref, field_out, lam_out, sem):
    copies = [pltpu.make_async_copy(field_ref, field_out, sem.at[0]),
              pltpu.make_async_copy(lam_ref, lam_out, sem.at[1])]
    for copy in copies:
        copy.start()
    for copy in copies:
        copy.wait()


def shards(shape, density, spread, sensitivities, violation, multipliers_start):
    nx, ny, nz = density.shape
    chunks = nx * ny // SUB
    groups = len(steps())
    stages = plan(shape)
    f32 = jnp.float32
    smem = pl.BlockSpec(memory_space=pltpu.SMEM)
    dma = pltpu.SemaphoreType.DMA
    hbm = pl.BlockSpec(memory_space=pltpu.HBM)
    anywhere = pl.BlockSpec(memory_space=pl.ANY)
    field, lam = pl.pallas_call(
        functools.partial(body, shape, (nx, ny, nz)),
        out_shape=(
            jax.ShapeDtypeStruct((nx, ny, nz), f32),
            jax.ShapeDtypeStruct((FIELDS,), f32),
        ),
        in_specs=[hbm] * 5,
        out_specs=(anywhere, smem),
        scratch_shapes=[
            pltpu.VMEM((nx, ny, nz), f32),
            pltpu.VMEM((nx, ny, nz), f32),
            pltpu.VMEM((nx, ny, nz), f32),
            pltpu.SMEM((FIELDS,), f32),
            pltpu.SMEM((FIELDS,), f32),
            pltpu.VMEM((FIELDS, nx + 2, ny + 2 * SUB, nz), f32),
            pltpu.VMEM((2, FIELDS, nx, nz), f32),
            pltpu.VMEM((2, FIELDS, nx, nz), f32),
            pltpu.VMEM((4, FIELDS, 1, nz), f32),
            pltpu.VMEM((4, FIELDS, 1, nz), f32),
            pltpu.VMEM((2, groups, SUB, LANE), f32),
            pltpu.VMEM((2, groups, SUB, LANE), f32),
            pltpu.VMEM((FIELDS, chunks, SUB, LANE), f32),
            pltpu.VMEM((chunks, SUB, LANE), f32),
            pltpu.VMEM((FIELDS + 1, chunks, SUB, LANE), f32),
            pltpu.VMEM((FIELDS + 1, chunks, SUB, LANE), f32),
            pltpu.VMEM((FIELDS, chunks, SUB, LANE), f32),
            pltpu.VMEM((FIELDS, chunks, SUB, LANE), f32),
            pltpu.VMEM((ROWS, SUB, LANE), f32),
            pltpu.VMEM((-(-ROWS // SUB), SUB, LANE), f32),
            pltpu.VMEM((FIELDS, SUB, LANE), f32),
            pltpu.VMEM((ITERS, len(stages), 1, LANE), f32),
        ] + [
            pltpu.VMEM((ITERS, math.prod(shape[a] for a in axes), 1, LANE), f32) for axes in stages
        ] + [
            dma((5,)), dma((6 + 4 * groups,)), dma((6 + 4 * groups,)),
            dma((ITERS, len(stages))), dma((ITERS, len(stages))), pltpu.SemaphoreType.REGULAR,
        ],
        compiler_params=pltpu.CompilerParams(
            collective_id=0, has_side_effects=True, vmem_limit_bytes=24 << 20),
        name="design_step",
    )(*[pltpu.with_memory_space_constraint(v, pltpu.HBM) for v in (density, spread, sensitivities, violation, multipliers_start)])
    return pl.pallas_call(
        finish,
        out_shape=(
            jax.ShapeDtypeStruct((nx, ny, nz), f32),
            jax.ShapeDtypeStruct((FIELDS,), f32),
        ),
        in_specs=[anywhere, anywhere],
        out_specs=(hbm, hbm),
        scratch_shapes=[dma((2,))],
        compiler_params=pltpu.CompilerParams(vmem_limit_bytes=1 << 20),
        name="finish",
    )(field, lam)


def solution(mesh):
    shape = {a: int(mesh.shape[a]) for a in AXES}
    return jax.shard_map(
        functools.partial(shards, shape),
        mesh=mesh,
        in_specs=(P("gx", "gy", "gz"), P("gx", "gy", "gz"), P(None, "gx", "gy", "gz"), P(), P()),
        out_specs=(P("gx", "gy", "gz"), P()),
        check_vma=False,
    )
```

```python
import functools
import math

import jax
import jax.numpy as jnp
from jax import lax
from jax.experimental import pallas as pl
from jax.experimental.pallas import tpu as pltpu
from jax.sharding import PartitionSpec as P

FIELDS = 9
ITERS = 3

RADIUS = 3.0
RAA = 1e-05
MOVE = 0.9
REG = 0.001
FLOOR = 0.2

W0 = RADIUS
W1 = RADIUS - 1.0
W2 = RADIUS - math.sqrt(2.0)
W3 = RADIUS - math.sqrt(3.0)

SUB, LANE = 8, 128
AXES = ("gz", "gy", "gx")
SUMS = FIELDS + FIELDS * (FIELDS + 1) // 2
ROWS = SUMS + FIELDS
MESH = pl.DeviceIdType.MESH
GROUP = 3


def plan(shape):
    total = math.prod(shape[a] for a in AXES)
    if total <= 32:
        return (AXES,)
    return tuple((a,) for a in AXES)


def offsets(axes, shape):
    out = [()]
    for a in axes:
        out = [o + (d,) for o in out for d in range(shape[a])]
    return [o for o in out if any(o)]


def steps():
    return [range(f, min(f + GROUP, FIELDS)) for f in range(0, FIELDS, GROUP)]


def body(shape, dims, dens_hbm, span_hbm, sens_ref, viol_hbm, lam0_hbm, out_hbm, lam_out,
         dens_ref, span_ref, out_ref, viol_ref, lam0_ref, pad, ypack, yrecv, cpack, crecv, zpack, zrecv, mid, invden, pp, qq, slope, scaled,
         acc, wide, lam, part, *rest):
    stages = plan(shape)
    recvs = rest[: len(stages)]
    load_sem, send_sem, recv_sem, sum_send, sum_recv, known = rest[len(stages):]
    nx, ny, nz = dims
    tiles = ny // SUB
    chunks = nx * tiles
    me = {a: lax.axis_index(a) for a in AXES}

    has = {}
    for a in AXES:
        has[a, -1] = me[a] > 0
        has[a, 0] = jnp.bool_(True)
        has[a, 1] = me[a] < shape[a] - 1

    def both(o):
        moved = [has[a, d] for a, d in zip(AXES, o) if d]
        return functools.reduce(jnp.logical_and, moved)

    def at(**moves):
        return {a: me[a] + d for a, d in moves.items()}

    plane = [(0, dy, dx) for dy in (-1, 0, 1) for dx in (-1, 0, 1) if dy or dx]
    barrier = pltpu.get_barrier_semaphore()
    near = shape["gz"] == 2 and shape["gy"] <= 4 and shape["gx"] <= 4
    if near:
        greeted = [(-1, 0, 0), (1, 0, 0)] + plane
        for o in greeted:
            @pl.when(both(o))
            def _(o=o):
                pl.semaphore_signal(barrier, inc=1, device_id=at(gz=o[0], gy=o[1], gx=o[2]),
                                    device_id_type=MESH)
        arrivals = sum(both(o).astype(jnp.int32) for o in greeted)
    else:
        partners = set()
        for axes in stages:
            for o in offsets(axes, shape):
                partners.add(tuple(dict(zip(axes, o)).get(a, 0) for a in AXES))
        for d in [(-1, 0, 0), (1, 0, 0)] + plane:
            o = tuple(d % shape[a] for a, d in zip(AXES, d))
            if any(o):
                partners.add(o)
        partners = sorted(partners)
        for o in partners:
            target = {a: lax.rem(me[a] + d, shape[a]) for a, d in zip(AXES, o)}
            pl.semaphore_signal(barrier, inc=1, device_id=target, device_id_type=MESH)
        arrivals = len(partners)

    load = pltpu.make_async_copy(
        sens_ref, pad.at[:, 1 : nx + 1, SUB : SUB + ny, :], load_sem.at[0]
    )
    load.start()
    small = [
        pltpu.make_async_copy(src, dst, load_sem.at[1 + i])
        for i, (src, dst) in enumerate([
            (span_hbm, span_ref), (dens_hbm, dens_ref), (viol_hbm, viol_ref), (lam0_hbm, lam0_ref)])
    ]
    for copy in small:
        copy.start()

    lane = lax.broadcasted_iota(jnp.int32, (SUB, LANE), 1)
    row = lax.broadcasted_iota(jnp.int32, (SUB, LANE), 0)
    zero = jnp.zeros((SUB, LANE), jnp.float32)

    for i, sx in enumerate((1, -1)):
        @pl.when(jnp.logical_not(has["gx", -sx]))
        def _(i=i):
            pad[:, i * (nx + 1), SUB : SUB + ny, :] = jnp.zeros((FIELDS, ny, LANE), jnp.float32)
    for i, sy in enumerate((1, -1)):
        @pl.when(jnp.logical_not(has["gy", -sy]))
        def _(i=i):
            yrecv[i] = jnp.zeros((FIELDS, nx, LANE), jnp.float32)
    for i, sz in enumerate((1, -1)):
        @pl.when(jnp.logical_not(has["gz", -sz]))
        def _(i=i):
            zrecv[i] = jnp.zeros(zrecv.shape[1:], jnp.float32)
    corners = [(sx, sy) for sx in (1, -1) for sy in (1, -1)]
    for i, (sx, sy) in enumerate(corners):
        @pl.when(jnp.logical_not(jnp.logical_and(has["gx", -sx], has["gy", -sy])))
        def _(i=i):
            crecv[i] = jnp.zeros((FIELDS, 1, LANE), jnp.float32)

    def count(a, index, extent):
        low = jnp.where(jnp.logical_and(me[a] == 0, index == 0), 0.0, 1.0)
        high = jnp.where(jnp.logical_and(me[a] == shape[a] - 1, index == extent - 1), 0.0, 1.0)
        return low + high
    cz = count("gz", lane, nz)
    for x in range(nx):
        cx = count("gx", jnp.full((SUB, LANE), x, jnp.int32), nx)
        for t in range(tiles):
            cy = count("gy", row + t * SUB, ny)
            den = W0 + W1 * (cx + cy + cz) + W2 * (cx * cy + cy * cz + cx * cz) + W3 * (cx * cy * cz)
            k = x * tiles + t
            invden[k] = 1.0 / den

    load.wait()

    for f in range(FIELDS):
        for i, y in enumerate((SUB + ny - 1, SUB)):
            for x in range(nx):
                ypack[i, f, x : x + 1, :] = pad[f, x + 1, y : y + 1, :]
        for i, (sx, sy) in enumerate(corners):
            x = nx if sx > 0 else 1
            y = SUB + ny - 1 if sy > 0 else SUB
            cpack[i, f] = pad[f, x, y : y + 1, :]

    pl.semaphore_wait(barrier, arrivals)

    groups = steps()
    count_of = len(groups)

    def moves_x(g):
        fields = pl.ds(groups[g][0], len(groups[g]))
        out = []
        for i, sx in enumerate((1, -1)):
            copy = pltpu.make_async_remote_copy(
                src_ref=pad.at[fields, nx if sx > 0 else 1, SUB : SUB + ny, :],
                dst_ref=pad.at[fields, 0 if sx > 0 else nx + 1, SUB : SUB + ny, :],
                send_sem=send_sem.at[6 + 4 * g + i], recv_sem=recv_sem.at[6 + 4 * g + i],
                device_id=at(gx=sx), device_id_type=MESH)
            out.append((has["gx", sx], has["gx", -sx], copy))
        return out

    moves_c, moves_y, moves_z = [], [], []
    for i, (sx, sy) in enumerate(corners):
        copy = pltpu.make_async_remote_copy(
            src_ref=cpack.at[i], dst_ref=crecv.at[i],
            send_sem=send_sem.at[2 + i], recv_sem=recv_sem.at[2 + i],
            device_id=at(gx=sx, gy=sy), device_id_type=MESH)
        moves_c.append((jnp.logical_and(has["gx", sx], has["gy", sy]),
                        jnp.logical_and(has["gx", -sx], has["gy", -sy]), copy))
    for i, sy in enumerate((1, -1)):
        copy = pltpu.make_async_remote_copy(
            src_ref=ypack.at[i], dst_ref=yrecv.at[i],
            send_sem=send_sem.at[i], recv_sem=recv_sem.at[i],
            device_id=at(gy=sy), device_id_type=MESH)
        moves_y.append((has["gy", sy], has["gy", -sy], copy))

    def start(moves):
        for send, _, copy in moves:
            pl.when(send)(copy.start)

    def receive(moves):
        for _, expected, copy in moves:
            pl.when(expected)(copy.wait_recv)

    xs = [moves_x(g) for g in range(count_of)]
    start(moves_c)
    start(xs[0])
    start(moves_y)
    for g in range(1, count_of):
        start(xs[g])
    receive(moves_c)
    receive(moves_y)

    ends = jnp.logical_or(lane == 0, lane == LANE - 1)

    def smooth(f, g):
        for i, y in enumerate((SUB - 1, SUB + ny)):
            for x in range(nx):
                pad[f, x + 1, y : y + 1, :] = yrecv[i, f, x : x + 1, :]
        for i, (sx, sy) in enumerate(corners):
            pad[f, 0 if sx > 0 else nx + 1, (SUB - 1 if sy > 0 else SUB + ny) : (SUB if sy > 0 else SUB + ny + 1), :] = crecv[i, f]
        packed = zero
        for t in range(tiles):
            y = SUB + t * SUB
            mids, sides = [], []
            for p in range(nx + 2):
                mids.append(pad[f, p, y : y + SUB, :])
                sides.append(pad[f, p, y - 1 : y - 1 + SUB, :] + pad[f, p, y + 1 : y + 1 + SUB, :])
            for x in range(nx):
                k = x * tiles + t
                near = sides[x + 1] + (mids[x] + mids[x + 2])
                far = sides[x] + sides[x + 2]
                s0 = W0 * mids[x + 1] + W1 * near + W2 * far
                s1 = W1 * mids[x + 1] + W2 * near + W3 * far
                up = pltpu.roll(s1, 1, 1)
                down = pltpu.roll(s1, LANE - 1, 1)
                mid[f, k] = s0 + jnp.where(lane == 0, 0.0, up) + jnp.where(lane == LANE - 1, 0.0, down)
                edge = jnp.where(lane == 0, up, down)
                if k:
                    edge = pltpu.roll(edge, 2 * k, 1)
                here = jnp.logical_or(lane == 2 * k, lane == (2 * k - 1) % LANE)
                packed = jnp.where(here, edge, packed)
        shift = (f - groups[g][0]) * (2 * chunks)
        return pltpu.roll(packed, shift, 1) if shift else packed

    even = (lane % 2) == 0
    for g in range(count_of):
        receive(xs[g])
        v = zero
        for f in groups[g]:
            v += smooth(f, g)
        zpack[0, g] = jnp.where(even, v, 0.0)
        zpack[1, g] = jnp.where(even, 0.0, v)
        zs = []
        for i, sz in enumerate((1, -1)):
            copy = pltpu.make_async_remote_copy(
                src_ref=zpack.at[i, g], dst_ref=zrecv.at[i, g],
                send_sem=send_sem.at[8 + 4 * g + i], recv_sem=recv_sem.at[8 + 4 * g + i],
                device_id=at(gz=sz), device_id_type=MESH)
            zs.append((has["gz", sz], has["gz", -sz], copy))
        start(zs)
        moves_z.append(zs)

    def piece(ref, k):
        x, t = divmod(k, tiles)
        return ref[x, t * SUB : (t + 1) * SUB, :]

    def rows(f, g):
        outer = zrecv[0, g] + zrecv[1, g]
        shift = (f - groups[g][0]) * (2 * chunks)
        total = zero
        for k in range(chunks):
            turn = (LANE - shift - 2 * k) % LANE
            edge = pltpu.roll(outer, turn, 1) if turn else outer
            r = (mid[f, k] + jnp.where(ends, edge, 0.0)) * invden[k]
            s = piece(span_ref, k)
            square = s * s
            gp = jnp.maximum(r, 0.0)
            gm = jnp.maximum(-r, 0.0)
            pp[f, k] = square * (1.001 * gp + 0.001 * gm + RAA)
            qq[f, k] = square * (0.001 * gp + 1.001 * gm + RAA)
            total += s * (1.002 * (gp + gm) + 2 * RAA)
        if f:
            acc[SUMS - 1 + f] = total

    for copy in small:
        copy.wait()
    for g in range(count_of):
        receive(moves_z[g])
        if near and g == 0:
            for o in plane:
                @pl.when(both(o))
                def _(o=o):
                    pl.semaphore_signal(known, inc=1, device_id=at(gy=o[1], gx=o[2]),
                                        device_id_type=MESH)
        for f in groups[g]:
            rows(f, g)
    total = zero
    for k in range(chunks):
        s = piece(span_ref, k)
        square = s * s
        pp[FIELDS, k] = square * (1.001 + RAA)
        qq[FIELDS, k] = square * (0.001 + RAA)
        total += s * (1.002 + 2 * RAA)
    acc[ROWS - 1] = total
    for k in range(FIELDS):
        lam[k] = jnp.full((SUB, LANE), lam0_ref[k], jnp.float32)

    def respond(k, weights):
        big_p, big_q = pp[0, k], qq[0, k]
        for j in range(FIELDS):
            big_p += weights[j] * pp[j + 1, k]
            big_q += weights[j] * qq[j + 1, k]
        s = piece(span_ref, k)
        d = piece(dens_ref, k)
        root_p = jnp.sqrt(big_p)
        root_q = jnp.sqrt(big_q)
        lower, upper = d - s, d + s
        moved = (root_p * lower + root_q * upper) / (root_p + root_q)
        low = jnp.maximum(0.0, d - MOVE * s)
        high = jnp.minimum(1.0, d + MOVE * s)
        return jnp.minimum(jnp.maximum(moved, low), high), big_p, big_q, lower, upper

    def flat(axes):
        index = 0
        for a in axes:
            index = index * shape[a] + me[a]
        return index

    def newton(it, carry):
        weights = [lam[j] for j in range(FIELDS)]
        grads = [zero] * FIELDS
        for k in range(chunks):
            moved, big_p, big_q, lower, upper = respond(k, weights)
            ia = 1.0 / (upper - moved)
            ib = 1.0 / (moved - lower)
            ia2, ib2 = ia * ia, ib * ib
            inv = 1.0 / (2.0 * big_p * (ia2 * ia) + 2.0 * big_q * (ib2 * ib))
            for j in range(FIELDS):
                p, q = pp[j + 1, k], qq[j + 1, k]
                grads[j] += p * ia + q * ib
                a = p * ia2 - q * ib2
                slope[j, k] = a
                scaled[j, k] = a * inv
        for j in range(FIELDS):
            acc[j] = grads[j]
        at_row = FIELDS
        for group in ((0, 1), (2, 3), (4, 5, 6, 7, 8)):
            sums = {(i, j): zero for i in group for j in range(i, FIELDS)}
            for k in range(chunks):
                right = {j: slope[j, k] for j in range(group[0], FIELDS)}
                for i in group:
                    left = scaled[i, k]
                    for j in range(i, FIELDS):
                        sums[i, j] += left * right[j]
            for key in sums:
                acc[at_row] = sums[key]
                at_row += 1

        packed = zero
        for r in range(ROWS):
            packed = jnp.where(lane == r, jnp.sum(acc[r], axis=1, keepdims=True), packed)
        value = jnp.sum(packed, axis=0, keepdims=True)
        for n, axes in enumerate(stages):
            size = math.prod(shape[a] for a in axes)
            part[it, n] = value
            recvs[n][it, flat(axes)] = value
            for o in sorted(offsets(axes, shape), key=lambda o: (-abs(o[-1] - 2), o), reverse=True):
                target = {a: lax.rem(me[a] + d, shape[a]) for a, d in zip(axes, o)}
                pltpu.make_async_remote_copy(
                    src_ref=part.at[it, n], dst_ref=recvs[n].at[it, flat(axes)],
                    send_sem=sum_send.at[it, n], recv_sem=sum_recv.at[it, n],
                    device_id=target, device_id_type=MESH).start()
            whole = recvs[n].at[it, pl.ds(0, size - 1)]
            pltpu.make_async_copy(whole, whole, sum_recv.at[it, n]).wait()
            values = [recvs[n][it, i] for i in range(size)]
            while len(values) > 1:
                values = [sum(values[i + 1 : i + 2], values[i]) for i in range(0, len(values), 2)]
            value = values[0]
        every = jnp.broadcast_to(value, (SUB, LANE))
        for g in range(wide.shape[0]):
            one = jnp.sum(jnp.where(lane == g * SUB + row, every, 0.0), axis=1, keepdims=True)
            wide[g] = jnp.broadcast_to(one, (SUB, LANE))

        def read(r):
            return jnp.broadcast_to(wide[r // SUB, r % SUB : r % SUB + 1, :], (SUB, LANE))
        b = [read(j) - (1.0 - viol_ref[j]) * read(SUMS + j) for j in range(FIELDS)]
        m = {}
        at_row = FIELDS
        for i in range(FIELDS):
            for j in range(i, FIELDS):
                m[i, j] = read(at_row)
                at_row += 1
        trace = m[0, 0]
        for i in range(1, FIELDS):
            trace += m[i, i]
        shift = REG * trace / FIELDS
        for i in range(FIELDS):
            m[i, i] += shift
        inverse = []
        for k in range(FIELDS):
            inverse.append(1.0 / m[k, k])
            for i in range(k + 1, FIELDS):
                factor = m[k, i] * inverse[k]
                for j in range(i, FIELDS):
                    m[i, j] -= factor * m[k, j]
                b[i] -= factor * b[k]
        delta = [None] * FIELDS
        for k in reversed(range(FIELDS)):
            v = b[k]
            for j in range(k + 1, FIELDS):
                v -= m[k, j] * delta[j]
            delta[k] = v * inverse[k]
        for k in range(FIELDS):
            lam[k] = jnp.maximum(weights[k] + delta[k], FLOOR * weights[k])
        return carry
    if near:
        pl.semaphore_wait(known, sum(both(o).astype(jnp.int32) for o in plane))
    lax.fori_loop(0, ITERS, newton, 0)

    weights = [lam[j] for j in range(FIELDS)]
    for k in range(chunks):
        x, t = divmod(k, tiles)
        out_ref[x, t * SUB : (t + 1) * SUB, :] = respond(k, weights)[0]
    result = pltpu.make_async_copy(out_ref, out_hbm, load_sem.at[0])
    result.start()
    for j in range(FIELDS):
        lam_out[j] = jnp.max(weights[j])

    for moves in [moves_c, moves_y] + xs + moves_z:
        for send, _, copy in moves:
            pl.when(send)(copy.wait_send)
    for it in range(ITERS):
        for n, axes in enumerate(stages):
            size = math.prod(shape[a] for a in axes)
            whole = recvs[n].at[it, pl.ds(0, size - 1)]
            pltpu.make_async_copy(whole, whole, sum_send.at[it, n]).wait()
    result.wait()


def finish(field_ref, lam_ref, field_out, lam_out, sem):
    copies = [pltpu.make_async_copy(field_ref, field_out, sem.at[0]),
              pltpu.make_async_copy(lam_ref, lam_out, sem.at[1])]
    for copy in copies:
        copy.start()
    for copy in copies:
        copy.wait()


def shards(shape, density, spread, sensitivities, violation, multipliers_start):
    nx, ny, nz = density.shape
    chunks = nx * ny // SUB
    groups = len(steps())
    stages = plan(shape)
    f32 = jnp.float32
    smem = pl.BlockSpec(memory_space=pltpu.SMEM)
    dma = pltpu.SemaphoreType.DMA
    hbm = pl.BlockSpec(memory_space=pltpu.HBM)
    anywhere = pl.BlockSpec(memory_space=pl.ANY)
    field, lam = pl.pallas_call(
        functools.partial(body, shape, (nx, ny, nz)),
        out_shape=(
            jax.ShapeDtypeStruct((nx, ny, nz), f32),
            jax.ShapeDtypeStruct((FIELDS,), f32),
        ),
        in_specs=[hbm] * 5,
        out_specs=(anywhere, smem),
        scratch_shapes=[
            pltpu.VMEM((nx, ny, nz), f32),
            pltpu.VMEM((nx, ny, nz), f32),
            pltpu.VMEM((nx, ny, nz), f32),
            pltpu.SMEM((FIELDS,), f32),
            pltpu.SMEM((FIELDS,), f32),
            pltpu.VMEM((FIELDS, nx + 2, ny + 2 * SUB, nz), f32),
            pltpu.VMEM((2, FIELDS, nx, nz), f32),
            pltpu.VMEM((2, FIELDS, nx, nz), f32),
            pltpu.VMEM((4, FIELDS, 1, nz), f32),
            pltpu.VMEM((4, FIELDS, 1, nz), f32),
            pltpu.VMEM((2, groups, SUB, LANE), f32),
            pltpu.VMEM((2, groups, SUB, LANE), f32),
            pltpu.VMEM((FIELDS, chunks, SUB, LANE), f32),
            pltpu.VMEM((chunks, SUB, LANE), f32),
            pltpu.VMEM((FIELDS + 1, chunks, SUB, LANE), f32),
            pltpu.VMEM((FIELDS + 1, chunks, SUB, LANE), f32),
            pltpu.VMEM((FIELDS, chunks, SUB, LANE), f32),
            pltpu.VMEM((FIELDS, chunks, SUB, LANE), f32),
            pltpu.VMEM((ROWS, SUB, LANE), f32),
            pltpu.VMEM((-(-ROWS // SUB), SUB, LANE), f32),
            pltpu.VMEM((FIELDS, SUB, LANE), f32),
            pltpu.VMEM((ITERS, len(stages), 1, LANE), f32),
        ] + [
            pltpu.VMEM((ITERS, math.prod(shape[a] for a in axes), 1, LANE), f32) for axes in stages
        ] + [
            dma((5,)), dma((6 + 4 * groups,)), dma((6 + 4 * groups,)),
            dma((ITERS, len(stages))), dma((ITERS, len(stages))), pltpu.SemaphoreType.REGULAR,
        ],
        compiler_params=pltpu.CompilerParams(
            collective_id=0, has_side_effects=True, vmem_limit_bytes=24 << 20),
        name="design_step",
    )(*[pltpu.with_memory_space_constraint(v, pltpu.HBM) for v in (density, spread, sensitivities, violation, multipliers_start)])
    return pl.pallas_call(
        finish,
        out_shape=(
            jax.ShapeDtypeStruct((nx, ny, nz), f32),
            jax.ShapeDtypeStruct((FIELDS,), f32),
        ),
        in_specs=[anywhere, anywhere],
        out_specs=(hbm, hbm),
        scratch_shapes=[dma((2,))],
        compiler_params=pltpu.CompilerParams(vmem_limit_bytes=1 << 20),
        name="finish",
    )(field, lam)


def solution(mesh):
    shape = {a: int(mesh.shape[a]) for a in AXES}
    return jax.shard_map(
        functools.partial(shards, shape),
        mesh=mesh,
        in_specs=(P("gx", "gy", "gz"), P("gx", "gy", "gz"), P(None, "gx", "gy", "gz"), P(), P()),
        out_specs=(P("gx", "gy", "gz"), P()),
        check_vma=False,
    )
```
